16 devices in a mesh: data: 4 (over z, y), expert: 4 (over x, core).
Axes of the slice: x: 2, y: 2, z: 2, core: 2. Of those that a mesh axis runs over, the one named last changes fastest.
Arguments:
- x_tok: bfloat16 [512, 2048], P(('data', 'expert')), parts along dimension 0
- topk_idx: int32 [512, 8], P(('data', 'expert')), parts along dimension 0
- topk_w: float32 [512, 8], P(('data', 'expert')), parts along dimension 0
- w_up: bfloat16 [64, 2048, 1024], P('expert')
- w_down: bfloat16 [64, 1024, 2048], P('expert')
Outputs:
- output: bfloat16 [512, 2048], P(('data', 'expert')), parts along dimension 0
There are 4 independent parts. The reference program is written for one: setup_inputs(seed, part) draws one part's arguments, and reference() takes and returns one part's arrays. A program takes and returns all parts, laid end to end along the dimension named above; an argument that names none is the same for every part.
All inputs are finite; a program needn't handle non-finite values.
Results may differ from the reference program's by a relative error of at most 0.00126.
Values are sent between devices in bfloat16 or wider.
A program may use at most 1 GiB of HBM per device.

```python
import jax
import jax.numpy as jnp
from jax import lax

D_MODEL = 2048
D_FF = 1024
EXPERTS = 64
TOP_K = 8
TOK_DEV = 32
GROUP_SIZE = 4
HOT_MUL = min(4, EXPERTS // TOP_K)
SLOT_CAP = HOT_MUL * TOK_DEV * TOP_K // EXPERTS
NUM_HOT = max(1, EXPERTS // 32)
TOKENS = GROUP_SIZE * TOK_DEV


def draw_routing(key):
    hot_key, dev_key = jax.random.split(key)
    exp_perm = jax.random.permutation(hot_key, EXPERTS)
    n_cold = EXPERTS - NUM_HOT
    cold_total = TOK_DEV * TOP_K - NUM_HOT * SLOT_CAP
    base_count = cold_total // n_cold
    extra_count = cold_total - base_count * n_cold

    def one_device(dev_seed):
        shift_key, order_key, perm_key = jax.random.split(dev_seed, 3)
        shifts = jax.random.randint(shift_key, (n_cold // 2,), 0, base_count // 2 + 1)
        count_shift = jnp.concatenate([jnp.stack([shifts, -shifts], axis=1).reshape(-1), jnp.zeros((n_cold % 2,), jnp.int32)])
        cold_counts = base_count + (jnp.arange(n_cold) < extra_count).astype(jnp.int32) + count_shift
        counts = jnp.concatenate([jnp.full((NUM_HOT,), SLOT_CAP, jnp.int32), cold_counts])
        visit_order = jax.random.permutation(order_key, EXPERTS)
        run_ends = jnp.cumsum(counts[visit_order])
        run_index = jnp.searchsorted(run_ends, jnp.arange(TOK_DEV * TOP_K), side='right')
        pair_seq = exp_perm[visit_order][run_index]
        choice = pair_seq.reshape(TOP_K, TOK_DEV).T
        return choice[jax.random.permutation(perm_key, TOK_DEV)]

    dev_keys = jax.random.split(dev_key, GROUP_SIZE)
    return jax.vmap(one_device)(dev_keys).reshape(TOKENS, TOP_K).astype(jnp.int32)


def setup_inputs(seed: int = 0, part: int = 0) -> dict:
    part_key = jax.random.fold_in(jax.random.key(seed), part)
    route_key, gate_key, tok_key = jax.random.split(part_key, 3)
    up_key, down_key = jax.random.split(jax.random.key(seed + 1))
    x_tok = jax.random.normal(tok_key, (TOKENS, D_MODEL), jnp.float32).astype(jnp.bfloat16)
    topk_idx = draw_routing(route_key)
    topk_w = jax.random.uniform(gate_key, (TOKENS, TOP_K), jnp.float32, 0.1, 1.0)
    w_up = (jax.random.normal(up_key, (EXPERTS, D_MODEL, D_FF), jnp.float32) * D_MODEL ** -0.5).astype(jnp.bfloat16)
    w_down = (jax.random.normal(down_key, (EXPERTS, D_FF, D_MODEL), jnp.float32) * D_FF ** -0.5).astype(jnp.bfloat16)
    return {'x_tok': x_tok, 'topk_idx': topk_idx, 'topk_w': topk_w, 'w_up': w_up, 'w_down': w_down}


def reference(x_tok, topk_idx, topk_w, w_up, w_down):
    pair_exp = topk_idx.reshape(-1)
    n_pairs = TOKENS * TOP_K
    group_cap = GROUP_SIZE * SLOT_CAP
    sort_order = jnp.argsort(pair_exp, stable=True)
    pair_rank = jnp.argsort(sort_order, stable=True)
    counts = jnp.bincount(pair_exp, length=EXPERTS)
    starts = jnp.cumsum(counts) - counts
    slot_src = jnp.minimum(starts[:, None] + jnp.arange(group_cap)[None, :], n_pairs - 1)
    slot_tok = sort_order[slot_src] // TOP_K

    def expert_rows(operands):
        tok_ids, up_mat, down_mat = operands
        tok_rows = x_tok[tok_ids]
        hidden = jnp.dot(tok_rows, up_mat, preferred_element_type=jnp.float32)
        hidden = jax.nn.gelu(hidden, approximate=True).astype(jnp.bfloat16)
        return jnp.dot(hidden, down_mat, preferred_element_type=jnp.float32).astype(jnp.bfloat16)

    slot_out = lax.map(expert_rows, (slot_tok, w_up, w_down)).reshape(EXPERTS * group_cap, D_MODEL)
    pair_slot = pair_exp * group_cap + pair_rank - starts[pair_exp]
    pair_out = slot_out[pair_slot].reshape(TOKENS, TOP_K, D_MODEL)
    y_tok = jnp.sum(topk_w[:, :, None] * pair_out.astype(jnp.float32), axis=1)
    return y_tok.astype(jnp.bfloat16)
```

```python
import functools

import jax
import jax.numpy as jnp
from jax import lax
from jax.experimental import pallas as pl
from jax.experimental.pallas import tpu as pltpu
from jax.sharding import PartitionSpec as P

MESH = pl.DeviceIdType.MESH
POOL = 2
RING = 24
SUB = 256
GELU_C = 0.7978845608028654


def gelu(v):
    return v * (0.5 + 0.5 * jnp.tanh(v * (GELU_C + (GELU_C * 0.044715) * (v * v))))


def kernel(pool, x_hbm, idx_hbm, gate_hbm, up_hbm, down_hbm, out_hbm,
           ring, xall, idx_all, gate_all, gb, hbuf, pacc, d2d_in, ssum, ici_in, out_v,
           ring_sem, load_sem, msend, mrecv, d2d_send, d2d_recv, ici_send, ici_recv, out_sem):
    data, expert = lax.axis_index("data"), lax.axis_index("expert")
    core = expert % 2
    y = data % pool
    chip = y * 2 + expert // 2
    me = chip * 2 + core
    chips = 2 * pool
    ranks = 2 * chips
    tok = x_hbm.shape[0]
    top_k = idx_hbm.shape[1]
    rows = ranks * tok
    n_loc = up_hbm.shape[0]
    n_exp = n_loc // pool
    width = ring.shape[3]
    half = ring.shape[2]
    n_up = up_hbm.shape[3] // width
    n_chunk = down_hbm.shape[2] // width
    n_pair = n_exp // 2
    up_items = n_exp * n_up
    items = up_items + n_chunk * n_pair
    first = y * n_exp

    partner = (data, expert + 1 - 2 * core)

    def chip_dev(k):
        ex = expert if k % 2 == 0 else lax.rem(expert + 2, 4)
        da = data if k < 2 else data + 1 - 2 * y
        return (da, ex)

    def up_copy(i):
        e, n = i // n_up, i % n_up
        return pltpu.make_async_copy(
            up_hbm.at[first + e, :, :, pl.ds(pl.multiple_of(n * width, width), width)],
            ring.at[i % RING], ring_sem.at[i % RING])

    def down_copy(i):
        j = i - up_items
        c, p = j // n_pair, j % n_pair
        return pltpu.make_async_copy(
            down_hbm.at[pl.ds(first + 2 * p, 2), :, pl.ds(pl.multiple_of(c * width, width), width)],
            ring.at[i % RING], ring_sem.at[i % RING])

    def fetch(i):
        @pl.when(i < up_items)
        def _():
            up_copy(i).start()

        @pl.when(jnp.logical_and(i >= up_items, i < items))
        def _():
            down_copy(i).start()

    def own(ref):
        return ref.at[pl.ds(pl.multiple_of(me * tok, tok), tok)]

    loads = [pltpu.make_async_copy(src, own(dst), load_sem.at[k])
             for k, (src, dst) in enumerate(((idx_hbm, idx_all), (gate_hbm, gate_all), (x_hbm, xall)))]
    for cp in loads:
        cp.start()
    for i in range(min(RING, items)):
        (up_copy if i < up_items else down_copy)(i).start()

    barrier = pltpu.get_barrier_semaphore()
    for dev in [partner] + [chip_dev(k) for k in range(1, chips)]:
        pl.semaphore_signal(barrier, inc=1, device_id=dev, device_id_type=MESH)
    pl.semaphore_wait(barrier, chips)

    def rank_rows(ref, r):
        return ref.at[pl.ds(pl.multiple_of(r * tok, tok), tok)]

    def send(ref, kind, r, slot, dev):
        return pltpu.make_async_remote_copy(
            src_ref=rank_rows(ref, r), dst_ref=rank_rows(ref, r),
            send_sem=msend.at[kind, slot], recv_sem=mrecv.at[kind, r],
            device_id=dev, device_id_type=MESH)

    bufs = (idx_all, gate_all, xall)
    other = [(chip ^ k) * 2 + core for k in range(chips)]
    started = []
    for kind, ref in enumerate(bufs):
        loads[kind].wait()
        for k in range(1, chips):
            cp = send(ref, kind, me, k - 1, chip_dev(k))
            cp.start()
            started.append(cp)
        cp = send(ref, kind, me, chips - 1, partner)
        cp.start()
        started.append(cp)
    for kind, ref in enumerate(bufs):
        for k in range(1, chips):
            send(ref, kind, other[k], 0, partner).wait_recv()
            cp = send(ref, kind, other[k], chips - 1 + k, partner)
            cp.start()
            started.append(cp)
        if kind == 1:
            for kk in range(2):
                for k in range(chips):
                    send(bufs[kk], kk, (chip ^ k) * 2 + 1 - core, 0, partner).wait_recv()
            for e in range(n_exp):
                eid = expert * n_loc + first + e
                hit = jnp.where(idx_all[...] == eid, gate_all[...], -1.0)
                gb[e] = jnp.broadcast_to(jnp.max(hit, axis=1, keepdims=True), (rows, 128))
    for k in range(chips):
        send(xall, 2, (chip ^ k) * 2 + 1 - core, 0, partner).wait_recv()

    def up_step(i, carry):
        e, n = i // n_up, i % n_up
        slot = i % RING
        up_copy(i).wait()
        keep = gb[e] >= 0.0
        for s in range(width // SUB):
            cols = pl.ds(s * SUB, SUB)
            acc = jnp.dot(xall[:, :half], ring[slot, 0, :, cols], preferred_element_type=jnp.float32)
            acc += jnp.dot(xall[:, half:], ring[slot, 1, :, cols], preferred_element_type=jnp.float32)
            for v in range(SUB // 128):
                part = gelu(acc[:, v * 128:(v + 1) * 128])
                hbuf[e, n, :, pl.ds(s * SUB + v * 128, 128)] = jnp.where(keep, part, 0.0).astype(jnp.bfloat16)
        fetch(i + RING)
        return carry

    lax.fori_loop(0, up_items, up_step, 0)

    def d2d(c):
        return pltpu.make_async_remote_copy(
            src_ref=pacc.at[c, :, 1 - core], dst_ref=d2d_in.at[c],
            send_sem=d2d_send.at[c], recv_sem=d2d_recv.at[c], device_id=partner, device_id_type=MESH)

    def ici(c, k):
        return pltpu.make_async_remote_copy(
            src_ref=ssum.at[c, chip ^ k], dst_ref=ici_in.at[c, k - 1],
            send_sem=ici_send.at[c, k - 1], recv_sem=ici_recv.at[c, k - 1],
            device_id=chip_dev(k), device_id_type=MESH)

    def forward(c):
        d2d(c).wait_recv()
        ssum[c] = pacc[c, :, core] + d2d_in[c]
        for k in range(chips - 1, 0, -1):
            ici(c, k).start()

    for c in range(n_chunk):
        def down_step(p, carry, c=c):
            i = up_items + c * n_pair + p
            slot = i % RING
            down_copy(i).wait()
            for s in range(width // SUB):
                cols = pl.ds(s * SUB, SUB)
                for b in range(2):
                    e = 2 * p + b
                    o = jnp.dot(hbuf[e, 0], ring[slot, b, :width, cols], preferred_element_type=jnp.float32)
                    for n in range(1, n_up):
                        o += jnp.dot(hbuf[e, n], ring[slot, b, n * width:(n + 1) * width, cols],
                                     preferred_element_type=jnp.float32)
                    o = o.astype(jnp.bfloat16).astype(jnp.float32)
                    for v in range(SUB // 128):
                        lane = pl.ds(s * SUB + v * 128, 128)
                        term = (gb[e] * o[:, v * 128:(v + 1) * 128]).reshape(chips, 2, tok, 128)
                        pacc[c, :, :, :, lane] += term
            fetch(i + RING)
            return carry

        pacc[c] = jnp.zeros(pacc.shape[1:], jnp.float32)
        lax.fori_loop(0, n_pair, down_step, 0)
        d2d(c).start()
        if c > 0:
            forward(c - 1)
    forward(n_chunk - 1)

    outs = []
    for c in range(n_chunk):
        total = ssum[c, chip]
        for k in range(1, chips):
            ici(c, k).wait_recv()
            total += ici_in[c, k - 1]
        out_v[c] = total.astype(jnp.bfloat16)
        cp = pltpu.make_async_copy(out_v.at[c], out_hbm.at[:, pl.ds(c * width, width)], out_sem.at[c])
        cp.start()
        outs.append(cp)
    for cp in started:
        cp.wait_send()
    for c in range(n_chunk):
        d2d(c).wait_send()
        for k in range(1, chips):
            ici(c, k).wait_send()
        outs[c].wait()


def solution(mesh):
    pool = POOL

    def local_moe(x_loc, idx_loc, gate_loc, up_loc, down_loc):
        tok, d_model = x_loc.shape
        top_k = idx_loc.shape[1]
        n_loc, _, d_ff = up_loc.shape
        chips, ranks = 2 * pool, 4 * pool
        rows = ranks * tok
        n_exp = n_loc // pool
        width = d_ff // 2
        n_chunk = d_model // width
        n_up = d_ff // width
        up4 = up_loc.reshape(n_loc, 2, d_model // 2, d_ff)
        dma, f32, bf16 = pltpu.SemaphoreType.DMA, jnp.float32, jnp.bfloat16
        hbm = pl.BlockSpec(memory_space=pltpu.HBM)
        return pl.pallas_call(
            functools.partial(kernel, pool),
            out_shape=jax.ShapeDtypeStruct((tok, d_model), bf16),
            in_specs=[hbm] * 5,
            out_specs=hbm,
            scratch_shapes=[
                pltpu.VMEM((RING, 2, d_ff, width), bf16),
                pltpu.VMEM((rows, d_model), bf16),
                pltpu.VMEM((rows, top_k), jnp.int32),
                pltpu.VMEM((rows, top_k), f32),
                pltpu.VMEM((n_exp, rows, 128), f32),
                pltpu.VMEM((n_exp, n_up, rows, width), bf16),
                pltpu.VMEM((n_chunk, chips, 2, tok, width), f32),
                pltpu.VMEM((n_chunk, chips, tok, width), f32),
                pltpu.VMEM((n_chunk, chips, tok, width), f32),
                pltpu.VMEM((n_chunk, chips - 1, tok, width), f32),
                pltpu.VMEM((n_chunk, tok, width), bf16),
                dma((RING,)), dma((3,)),
                dma((3, 2 * chips - 1)), dma((3, ranks)),
                dma((n_chunk,)), dma((n_chunk,)),
                dma((n_chunk, chips - 1)), dma((n_chunk, chips - 1)),
                dma((n_chunk,)),
            ],
            compiler_params=pltpu.CompilerParams(
                collective_id=0, has_side_effects=True, vmem_limit_bytes=67043328),
            name="moe",
        )(x_loc, idx_loc, gate_loc, up4, down_loc)

    tok_spec = P(('data', 'expert'), None)
    w_spec = P('expert', None, None)
    return jax.shard_map(local_moe, mesh=mesh, in_specs=(tok_spec, tok_spec, tok_spec, w_spec, w_spec), out_specs=tok_spec, check_vma=False)
```

```python
import functools

import jax
import jax.numpy as jnp
from jax import lax
from jax.experimental import pallas as pl
from jax.experimental.pallas import tpu as pltpu
from jax.sharding import PartitionSpec as P

MESH = pl.DeviceIdType.MESH
POOL = 2
RING = 22
SUB = 256
GELU_C = 0.7978845608028654


def gelu(v):
    return v * (0.5 + 0.5 * jnp.tanh(v * (GELU_C + (GELU_C * 0.044715) * (v * v))))


def kernel(pool, cap, x_hbm, idx_hbm, gate_hbm, up_hbm, down_hbm, out_hbm,
           ring, xall, idx_all, gate_all, pmat, cmat, xg, hbuf, obuf, pacc, d2d_in, ssum, ici_in, out_v,
           ring_sem, load_sem, msend, mrecv, d2d_send, d2d_recv, ici_send, ici_recv, out_sem):
    data, expert = lax.axis_index("data"), lax.axis_index("expert")
    core = expert % 2
    y = data % pool
    chips = 2 * pool
    ranks = 2 * chips
    tok = x_hbm.shape[0]
    top_k = idx_hbm.shape[0]
    n_loc = up_hbm.shape[0]
    n_exp = n_loc // pool
    width = ring.shape[3]
    half = ring.shape[2]
    n_up = up_hbm.shape[3] // width
    n_chunk = down_hbm.shape[2] // width
    n_pair = n_exp // 2
    up_items = n_exp * n_up
    items = up_items + n_chunk * n_pair
    first = y * n_exp
    slots = n_exp * cap

    partner = (data, expert + 1 - 2 * core)

    def chip_dev(k):
        ex = expert if k % 2 == 0 else lax.rem(expert + 2, 4)
        da = data if k < 2 else data + 1 - 2 * y
        return (da, ex)

    def up_copy(i):
        e, n = i // n_up, i % n_up
        return pltpu.make_async_copy(
            up_hbm.at[first + e, :, :, pl.ds(pl.multiple_of(n * width, width), width)],
            ring.at[i % RING], ring_sem.at[i % RING])

    def down_copy(i):
        j = i - up_items
        c, p = j // n_pair, j % n_pair
        return pltpu.make_async_copy(
            down_hbm.at[pl.ds(first + 2 * p, 2), :, pl.ds(pl.multiple_of(c * width, width), width)],
            ring.at[i % RING], ring_sem.at[i % RING])

    def fetch(i):
        @pl.when(i < up_items)
        def _():
            up_copy(i).start(priority=1)

        @pl.when(jnp.logical_and(i >= up_items, i < items))
        def _():
            down_copy(i).start(priority=1)

    bufs = (idx_all, gate_all, xall)
    loads = [pltpu.make_async_copy(src, dst.at[0], load_sem.at[k])
             for k, (src, dst) in enumerate(zip((idx_hbm, gate_hbm, x_hbm), bufs))]
    for cp in loads:
        cp.start()
    for i in range(min(RING, items)):
        (up_copy if i < up_items else down_copy)(i).start(priority=1)

    barrier = pltpu.get_barrier_semaphore()
    for dev in [partner] + [chip_dev(k) for k in range(1, chips)]:
        pl.semaphore_signal(barrier, inc=1, device_id=dev, device_id_type=MESH)
    pl.semaphore_wait(barrier, chips)

    started = []

    def send(kind, src, dst, dev):
        cp = pltpu.make_async_remote_copy(
            src_ref=bufs[kind].at[src], dst_ref=bufs[kind].at[dst],
            send_sem=msend.at[kind, dst - 1], recv_sem=mrecv.at[kind, dst],
            device_id=dev, device_id_type=MESH)
        cp.start()
        started.append(cp)

    def arrived(kind, src):
        pltpu.make_async_remote_copy(
            src_ref=bufs[kind].at[src], dst_ref=bufs[kind].at[src],
            send_sem=msend.at[kind, 0], recv_sem=mrecv.at[kind, src],
            device_id=partner, device_id_type=MESH).wait_recv()

    for kind in range(3):
        loads[kind].wait()
        for k in range(chips - 1, 0, -1):
            send(kind, 0, 2 * k, chip_dev(k))
        send(kind, 0, 1, partner)
    for kind in range(2):
        for k in range(1, chips):
            arrived(kind, 2 * k)
            send(kind, 2 * k, 2 * k + 1, partner)
    for kind in range(2):
        for k in range(chips):
            arrived(kind, 2 * k + 1)

    row = lax.broadcasted_iota(jnp.int32, (slots, tok), 0)
    eid = row // cap + (expert * n_loc + first)
    pos = (row % cap).astype(jnp.float32)
    before = (lax.broadcasted_iota(jnp.int32, (tok, tok), 0)
              < lax.broadcasted_iota(jnp.int32, (tok, tok), 1)).astype(jnp.bfloat16)
    for r in range(ranks):
        chose = jnp.zeros((slots, tok), jnp.float32)
        gate = jnp.zeros((slots, tok), jnp.float32)
        for j in range(top_k):
            hit = idx_all[r, j:j + 1, :] == eid
            chose = jnp.where(hit, 1.0, chose)
            gate = jnp.where(hit, gate_all[r, j:j + 1, :], gate)
        seen = jnp.dot(chose.astype(jnp.bfloat16), before, preferred_element_type=jnp.float32)
        one = jnp.logical_and(chose > 0.0, seen == pos)
        pmat[r] = jnp.where(one, 1.0, 0.0).astype(jnp.bfloat16)
        comb = jnp.where(one, gate, 0.0).T
        hi = comb.astype(jnp.bfloat16)
        rest = comb - hi.astype(jnp.float32)
        mid = rest.astype(jnp.bfloat16)
        low = (rest - mid.astype(jnp.float32)).astype(jnp.bfloat16)
        cmat[r, 0:tok] = hi
        cmat[r, tok:2 * tok] = mid
        cmat[r, 2 * tok:] = low

    def gather(r):
        for s in range(xall.shape[2] // SUB):
            cols = slice(s * SUB, (s + 1) * SUB)
            rows = jnp.dot(pmat[r], xall[r, :, cols], preferred_element_type=jnp.float32)
            xg[:, r * cap:(r + 1) * cap, cols] = rows.astype(jnp.bfloat16).reshape(n_exp, cap, SUB)

    gather(0)
    arrived(2, 1)
    gather(1)
    for k in range(1, chips):
        arrived(2, 2 * k)
        send(2, 2 * k, 2 * k + 1, partner)
        gather(2 * k)
    for k in range(1, chips):
        arrived(2, 2 * k + 1)
        gather(2 * k + 1)

    def up_step(e, carry):
        for n in range(n_up):
            i = e * n_up + n
            slot = i % RING
            up_copy(i).wait()
            for s in range(width // SUB):
                cols = slice(s * SUB, (s + 1) * SUB)
                acc = jnp.dot(xg[e, :, :half], ring[slot, 0, :, cols], preferred_element_type=jnp.float32)
                acc += jnp.dot(xg[e, :, half:], ring[slot, 1, :, cols], preferred_element_type=jnp.float32)
                hbuf[e, n, :, cols] = gelu(acc).astype(jnp.bfloat16)
            fetch(i + RING)
        return carry

    lax.fori_loop(0, n_exp, up_step, 0)

    def d2d(c):
        return pltpu.make_async_remote_copy(
            src_ref=pacc.at[c, 1], dst_ref=d2d_in.at[c],
            send_sem=d2d_send.at[c], recv_sem=d2d_recv.at[c], device_id=partner, device_id_type=MESH)

    def ici(c, k):
        return pltpu.make_async_remote_copy(
            src_ref=ssum.at[c, k], dst_ref=ici_in.at[c, k - 1],
            send_sem=ici_send.at[c, k - 1], recv_sem=ici_recv.at[c, k - 1],
            device_id=chip_dev(k), device_id_type=MESH)

    def forward(c):
        d2d(c).wait_recv()
        ssum[c] = pacc[c, 0] + d2d_in[c]
        for k in range(chips - 1, 0, -1):
            ici(c, k).start()

    for c in range(n_chunk):
        for p in range(n_pair):
            i = up_items + c * n_pair + p
            slot = i % RING
            down_copy(i).wait()
            for s in range(width // SUB):
                cols = slice(s * SUB, (s + 1) * SUB)
                for b in range(2):
                    e = 2 * p + b
                    o = jnp.dot(hbuf[e, 0], ring[slot, b, :width, cols], preferred_element_type=jnp.float32)
                    for n in range(1, n_up):
                        o += jnp.dot(hbuf[e, n], ring[slot, b, n * width:(n + 1) * width, cols],
                                     preferred_element_type=jnp.float32)
                    obuf[e, :, cols] = o.astype(jnp.bfloat16)
            if i + RING < items:
                fetch(i + RING)
        for s in range(width // SUB):
            cols = slice(s * SUB, (s + 1) * SUB)
            for r in range(ranks):
                o = obuf[:, r * cap:(r + 1) * cap, cols].reshape(slots, SUB)
                t = jnp.dot(cmat[r], o, preferred_element_type=jnp.float32)
                pacc[c, r % 2, r // 2, :, cols] = t[:tok] + t[tok:2 * tok] + t[2 * tok:]
        d2d(c).start()
        if c > 0:
            forward(c - 1)
    forward(n_chunk - 1)

    outs = []
    for c in range(n_chunk):
        total = ssum[c, 0]
        for k in range(1, chips):
            ici(c, k).wait_recv()
            total += ici_in[c, k - 1]
        out_v[c] = total.astype(jnp.bfloat16)
        cp = pltpu.make_async_copy(out_v.at[c], out_hbm.at[:, pl.ds(c * width, width)], out_sem.at[c])
        cp.start()
        outs.append(cp)
    for cp in started:
        cp.wait_send()
    for c in range(n_chunk):
        d2d(c).wait_send()
        for k in range(1, chips):
            ici(c, k).wait_send()
        outs[c].wait()


def solution(mesh):
    pool = POOL

    def local_moe(x_loc, idx_loc, gate_loc, up_loc, down_loc):
        tok, d_model = x_loc.shape
        top_k = idx_loc.shape[1]
        n_loc, _, d_ff = up_loc.shape
        n_all = n_loc * mesh.shape['expert']
        cap = min(4, n_all // top_k) * tok * top_k // n_all
        chips, ranks = 2 * pool, 4 * pool
        n_exp = n_loc // pool
        slots = n_exp * cap
        width = d_ff // 2
        n_chunk = d_model // width
        n_up = d_ff // width
        up4 = up_loc.reshape(n_loc, 2, d_model // 2, d_ff)
        dma, f32, bf16 = pltpu.SemaphoreType.DMA, jnp.float32, jnp.bfloat16
        hbm = pl.BlockSpec(memory_space=pltpu.HBM)
        return pl.pallas_call(
            functools.partial(kernel, pool, cap),
            out_shape=jax.ShapeDtypeStruct((tok, d_model), bf16),
            in_specs=[hbm] * 5,
            out_specs=hbm,
            scratch_shapes=[
                pltpu.VMEM((RING, 2, d_ff, width), bf16),
                pltpu.VMEM((ranks, tok, d_model), bf16),
                pltpu.VMEM((ranks, top_k, tok), jnp.int32),
                pltpu.VMEM((ranks, top_k, tok), f32),
                pltpu.VMEM((ranks, slots, tok), bf16),
                pltpu.VMEM((ranks, 3 * tok, slots), bf16),
                pltpu.VMEM((n_exp, ranks * cap, d_model), bf16),
                pltpu.VMEM((n_exp, n_up, ranks * cap, width), bf16),
                pltpu.VMEM((n_exp, ranks * cap, width), bf16),
                pltpu.VMEM((n_chunk, 2, chips, tok, width), f32),
                pltpu.VMEM((n_chunk, chips, tok, width), f32),
                pltpu.VMEM((n_chunk, chips, tok, width), f32),
                pltpu.VMEM((n_chunk, chips - 1, tok, width), f32),
                pltpu.VMEM((n_chunk, tok, width), bf16),
                dma((RING,)), dma((3,)),
                dma((3, ranks - 1)), dma((3, ranks)),
                dma((n_chunk,)), dma((n_chunk,)),
                dma((n_chunk, chips - 1)), dma((n_chunk, chips - 1)),
                dma((n_chunk,)),
            ],
            compiler_params=pltpu.CompilerParams(
                collective_id=0, has_side_effects=True, vmem_limit_bytes=67043328),
            name="moe",
        )(x_loc, idx_loc.T, gate_loc.T, up4, down_loc)

    tok_spec = P(('data', 'expert'), None)
    w_spec = P('expert', None, None)
    return jax.shard_map(local_moe, mesh=mesh, in_specs=(tok_spec, tok_spec, tok_spec, w_spec, w_spec), out_specs=tok_spec, check_vma=False)
```

```python
import functools

import jax
import jax.numpy as jnp
from jax import lax
from jax.experimental import pallas as pl
from jax.experimental.pallas import tpu as pltpu
from jax.sharding import PartitionSpec as P

MESH = pl.DeviceIdType.MESH
POOL = 2
RING = 20
SUB = 256
GELU_C = 0.7978845608028654


def gelu(v):
    return v * (0.5 + 0.5 * jnp.tanh(v * (GELU_C + (GELU_C * 0.044715) * (v * v))))


def kernel(pool, cap, x_hbm, idx_hbm, gate_hbm, up_hbm, down_hbm, out_hbm,
           ring, xall, idx_all, gate_all, pmat, cmat, xg, part, hbuf, obuf, pacc, d2d_in, ssum, ici_in, out_v,
           ring_sem, load_sem, msend, mrecv, d2d_send, d2d_recv, ici_send, ici_recv, out_sem):
    data, expert = lax.axis_index("data"), lax.axis_index("expert")
    core = expert % 2
    y = data % pool
    chips = 2 * pool
    ranks = 2 * chips
    tok = x_hbm.shape[0]
    top_k = idx_hbm.shape[0]
    n_loc = up_hbm.shape[0]
    n_exp = n_loc // pool
    half, width = ring.shape[2:]
    n_up = up_hbm.shape[3] // width
    n_wide = down_hbm.shape[2] // width
    n_chunk = down_hbm.shape[2] // SUB
    n_pair = n_exp // 2
    half_items = n_pair * n_up
    up_items = 2 * half_items
    items = up_items + n_wide * n_pair
    first = y * n_exp
    slots = n_exp * cap

    partner = (data, expert + 1 - 2 * core)

    def chip_dev(k):
        ex = expert if k % 2 == 0 else lax.rem(expert + 2, 4)
        da = data if k < 2 else data + 1 - 2 * y
        return (da, ex)

    def weight(i):
        if i < up_items:
            k, p, n = i // half_items, i % half_items // n_up, i % n_up
            src = up_hbm.at[pl.ds(first + 2 * p, 2), k, :, pl.ds(n * width, width)]
        else:
            c, p = (i - up_items) // n_pair, (i - up_items) % n_pair
            src = down_hbm.at[pl.ds(first + 2 * p, 2), :, pl.ds(c * width, width)]
        return pltpu.make_async_copy(src, ring.at[i % RING], ring_sem.at[i % RING])

    def buf(kind, r):
        return (idx_all, gate_all)[kind].at[r] if kind < 2 else xall.at[kind - 2, r]

    loads = [pltpu.make_async_copy(src, buf(k, 0), load_sem.at[k])
             for k, src in enumerate((idx_hbm, gate_hbm, x_hbm.at[:, :half], x_hbm.at[:, half:]))]
    for cp in loads:
        cp.start()
    for i in range(min(RING, items)):
        weight(i).start(priority=1)

    barrier = pltpu.get_barrier_semaphore()
    for dev in [partner] + [chip_dev(k) for k in range(1, chips)]:
        pl.semaphore_signal(barrier, inc=1, device_id=dev, device_id_type=MESH)
    pl.semaphore_wait(barrier, chips)

    started = []

    def remote(kind, src, dst, dev):
        return pltpu.make_async_remote_copy(
            src_ref=buf(kind, src), dst_ref=buf(kind, dst),
            send_sem=msend.at[kind, dst - 1], recv_sem=mrecv.at[kind, dst],
            device_id=dev, device_id_type=MESH)

    def send(kind, src, dst, dev):
        cp = remote(kind, src, dst, dev)
        cp.start()
        started.append(cp)

    def arrived(kind, r):
        remote(kind, r, r, partner).wait_recv()

    def relay(kind, k):
        arrived(kind, 2 * k)
        send(kind, 2 * k, 2 * k + 1, partner)

    far_first = list(range(chips - 1, 0, -1))
    for kind in range(4):
        loads[kind].wait()
        for k in far_first:
            send(kind, 0, 2 * k, chip_dev(k))
        send(kind, 0, 1, partner)
    for kind in range(2):
        for k in range(1, chips):
            relay(kind, k)
    for kind in range(2):
        for k in range(chips):
            arrived(kind, 2 * k + 1)

    row = lax.broadcasted_iota(jnp.int32, (slots, tok), 0)
    eid = row // cap + (expert * n_loc + first)
    pos = (row % cap).astype(jnp.float32)
    before = (lax.broadcasted_iota(jnp.int32, (tok, tok), 0)
              < lax.broadcasted_iota(jnp.int32, (tok, tok), 1)).astype(jnp.bfloat16)
    for r in range(ranks):
        chose = jnp.zeros((slots, tok), jnp.float32)
        gate = jnp.zeros((slots, tok), jnp.float32)
        for j in range(top_k):
            hit = idx_all[r, j:j + 1, :] == eid
            chose = jnp.where(hit, 1.0, chose)
            gate = jnp.where(hit, gate_all[r, j:j + 1, :], gate)
        seen = jnp.dot(chose.astype(jnp.bfloat16), before, preferred_element_type=jnp.float32)
        one = jnp.logical_and(chose > 0.0, seen == pos)
        pmat[r] = jnp.where(one, 1.0, 0.0).astype(jnp.bfloat16)
        comb = jnp.where(one, gate, 0.0).T
        hi = comb.astype(jnp.bfloat16)
        rest = comb - hi.astype(jnp.float32)
        mid = rest.astype(jnp.bfloat16)
        low = (rest - mid.astype(jnp.float32)).astype(jnp.bfloat16)
        cmat[r, 0:tok] = hi
        cmat[r, tok:2 * tok] = mid
        cmat[r, 2 * tok:] = low

    def gather(k, r):
        for s in range(half // SUB):
            cols = slice(s * SUB, (s + 1) * SUB)
            rows = jnp.dot(pmat[r], xall[k, r, :, cols], preferred_element_type=jnp.float32)
            xg[k, :, r * cap:(r + 1) * cap, cols] = rows.astype(jnp.bfloat16).reshape(n_exp, cap, SUB)

    def up_dot(k, p, b, n, cols):
        slot = k * half_items + p * n_up + n
        return jnp.dot(xg[k, 2 * p + b], ring[slot, b, :, cols], preferred_element_type=jnp.float32)

    def up_first(p, carry):
        for b in range(2):
            for n in range(n_up):
                for s in range(width // SUB):
                    cols = slice(s * SUB, (s + 1) * SUB)
                    part[2 * p + b, n, :, cols] = up_dot(0, p, b, n, cols)
        return carry

    def up_second(p, carry):
        for b in range(2):
            for n in range(n_up):
                for s in range(width // SUB):
                    cols = slice(s * SUB, (s + 1) * SUB)
                    acc = part[2 * p + b, n, :, cols] + up_dot(1, p, b, n, cols)
                    hbuf[2 * p + b, n, :, cols] = gelu(acc).astype(jnp.bfloat16)
        return carry

    gather(0, 0)
    arrived(2, 1)
    gather(0, 1)
    for k in range(1, chips):
        relay(2, k)
        gather(0, 2 * k)
    for k in range(1, chips):
        arrived(2, 2 * k + 1)
        gather(0, 2 * k + 1)
    for i in range(half_items):
        weight(i).wait()
    lax.fori_loop(0, n_pair // 2, up_first, 0)
    for k in range(1, chips - 1):
        relay(3, k)
    lax.fori_loop(n_pair // 2, n_pair, up_first, 0)
    for i in range(RING, min(RING + half_items, items)):
        weight(i).start(priority=1)
    relay(3, chips - 1)
    gather(1, 0)
    arrived(3, 1)
    gather(1, 1)
    for k in range(1, chips):
        gather(1, 2 * k)
    for k in range(1, chips):
        arrived(3, 2 * k + 1)
        gather(1, 2 * k + 1)
    for i in range(half_items, up_items):
        weight(i).wait()
    lax.fori_loop(0, n_pair, up_second, 0)
    for i in range(RING + half_items, min(RING + up_items, items)):
        weight(i).start(priority=1)

    def d2d(c):
        return pltpu.make_async_remote_copy(
            src_ref=pacc.at[c, 1], dst_ref=d2d_in.at[c],
            send_sem=d2d_send.at[c], recv_sem=d2d_recv.at[c], device_id=partner, device_id_type=MESH)

    def ici(c, k):
        return pltpu.make_async_remote_copy(
            src_ref=ssum.at[c, k], dst_ref=ici_in.at[c, k - 1],
            send_sem=ici_send.at[c, k - 1], recv_sem=ici_recv.at[c, k - 1],
            device_id=chip_dev(k), device_id_type=MESH)

    def forward(c):
        d2d(c).wait_recv()
        ssum[c] = pacc[c, 0] + d2d_in[c]
        for k in far_first:
            ici(c, k).start()

    for c in range(n_chunk):
        wide, s = c * SUB // width, c * SUB % width
        cols = slice(s, s + SUB)
        base = up_items + wide * n_pair
        if s == 0:
            for p in range(n_pair):
                weight(base + p).wait()
        for e in range(n_exp):
            slot = (base + e // 2) % RING
            o = jnp.dot(hbuf[e, 0], ring[slot, e % 2, :width, cols], preferred_element_type=jnp.float32)
            for n in range(1, n_up):
                o += jnp.dot(hbuf[e, n], ring[slot, e % 2, n * width:(n + 1) * width, cols],
                             preferred_element_type=jnp.float32)
            obuf[e] = o.astype(jnp.bfloat16)
        for r in range(ranks):
            o = obuf[:, r * cap:(r + 1) * cap, :].reshape(slots, SUB)
            t = jnp.dot(cmat[r], o, preferred_element_type=jnp.float32)
            pacc[c, r % 2, r // 2] = t[:tok] + t[tok:2 * tok] + t[2 * tok:]
        d2d(c).start()
        if c > 0:
            forward(c - 1)
    forward(n_chunk - 1)

    outs = []
    for c in range(n_chunk):
        total = ssum[c, 0]
        for k in range(1, chips):
            ici(c, k).wait_recv()
            total += ici_in[c, k - 1]
        out_v[c] = total.astype(jnp.bfloat16)
        cp = pltpu.make_async_copy(out_v.at[c], out_hbm.at[:, pl.ds(c * SUB, SUB)], out_sem.at[c])
        cp.start()
        outs.append(cp)
    for cp in started:
        cp.wait_send()
    for c in range(n_chunk):
        d2d(c).wait_send()
        for k in range(1, chips):
            ici(c, k).wait_send()
        outs[c].wait()


def solution(mesh):
    pool = POOL

    def local_moe(x_loc, idx_loc, gate_loc, up_loc, down_loc):
        tok, d_model = x_loc.shape
        top_k = idx_loc.shape[1]
        n_loc, _, d_ff = up_loc.shape
        n_all = n_loc * mesh.shape['expert']
        cap = min(4, n_all // top_k) * tok * top_k // n_all
        chips, ranks = 2 * pool, 4 * pool
        n_exp = n_loc // pool
        slots = n_exp * cap
        width = d_ff // 2
        n_chunk = d_model // SUB
        n_up = d_ff // width
        up4 = up_loc.reshape(n_loc, 2, d_model // 2, d_ff)
        dma, f32, bf16 = pltpu.SemaphoreType.DMA, jnp.float32, jnp.bfloat16
        hbm = pl.BlockSpec(memory_space=pltpu.HBM)
        return pl.pallas_call(
            functools.partial(kernel, pool, cap),
            out_shape=jax.ShapeDtypeStruct((tok, d_model), bf16),
            in_specs=[hbm] * 5,
            out_specs=hbm,
            scratch_shapes=[
                pltpu.VMEM((RING, 2, d_ff, width), bf16),
                pltpu.VMEM((2, ranks, tok, d_model // 2), bf16),
                pltpu.VMEM((ranks, top_k, tok), jnp.int32),
                pltpu.VMEM((ranks, top_k, tok), f32),
                pltpu.VMEM((ranks, slots, tok), bf16),
                pltpu.VMEM((ranks, 3 * tok, slots), bf16),
                pltpu.VMEM((2, n_exp, ranks * cap, d_model // 2), bf16),
                pltpu.VMEM((n_exp, n_up, ranks * cap, width), f32),
                pltpu.VMEM((n_exp, n_up, ranks * cap, width), bf16),
                pltpu.VMEM((n_exp, ranks * cap, SUB), bf16),
                pltpu.VMEM((n_chunk, 2, chips, tok, SUB), f32),
                pltpu.VMEM((n_chunk, chips, tok, SUB), f32),
                pltpu.VMEM((n_chunk, chips, tok, SUB), f32),
                pltpu.VMEM((n_chunk, chips - 1, tok, SUB), f32),
                pltpu.VMEM((n_chunk, tok, SUB), bf16),
                dma((RING,)), dma((4,)),
                dma((4, ranks - 1)), dma((4, ranks)),
                dma((n_chunk,)), dma((n_chunk,)),
                dma((n_chunk, chips - 1)), dma((n_chunk, chips - 1)),
                dma((n_chunk,)),
            ],
            compiler_params=pltpu.CompilerParams(
                collective_id=0, has_side_effects=True, vmem_limit_bytes=67043328),
            name="moe",
        )(x_loc, idx_loc.T, gate_loc.T, up4, down_loc)

    tok_spec = P(('data', 'expert'), None)
    w_spec = P('expert', None, None)
    return jax.shard_map(local_moe, mesh=mesh, in_specs=(tok_spec, tok_spec, tok_spec, w_spec, w_spec), out_specs=tok_spec, check_vma=False)
```

```python
import functools

import jax
import jax.numpy as jnp
from jax import lax
from jax.experimental import pallas as pl
from jax.experimental.pallas import tpu as pltpu
from jax.sharding import PartitionSpec as P

MESH = pl.DeviceIdType.MESH
POOL = 2
RING = 20
SUB = 256
STAGED = 7
LAG = 4
GELU_C = 0.7978845608028654


def gelu(v):
    return v * (0.5 + 0.5 * jnp.tanh(v * (GELU_C + (GELU_C * 0.044715) * (v * v))))


def kernel(pool, cap, x_hbm, idx_hbm, gate_hbm, up_hbm, down_hbm, out_hbm,
           ring, xall, idx_all, gate_all, pmat, cmat, xg, part, hbuf, obuf, pacc, d2d_in, ssum, ici_in, out_v,
           ring_sem, load_sem, msend, mrecv, d2d_send, d2d_recv, ici_send, ici_recv, out_sem):
    data, expert = lax.axis_index("data"), lax.axis_index("expert")
    core = expert % 2
    y = data % pool
    chips = 2 * pool
    ranks = 2 * chips
    tok = x_hbm.shape[0]
    top_k = idx_hbm.shape[0]
    n_loc = up_hbm.shape[0]
    n_exp = n_loc // pool
    half, width = ring.shape[2:]
    n_up = up_hbm.shape[3] // width
    n_wide = down_hbm.shape[2] // width
    n_chunk = down_hbm.shape[2] // SUB
    n_pair = n_exp // 2
    half_items = n_pair * n_up
    up_items = 2 * half_items
    items = up_items + n_wide * n_pair
    first = y * n_exp
    slots = n_exp * cap

    partner = (data, expert + 1 - 2 * core)

    def chip_dev(k):
        ex = expert if k % 2 == 0 else lax.rem(expert + 2, 4)
        da = data if k < 2 else data + 1 - 2 * y
        return (da, ex)

    def weight(i):
        if i < up_items:
            k, p, n = i // half_items, i % half_items // n_up, i % n_up
            src = up_hbm.at[pl.ds(first + 2 * p, 2), k, :, pl.ds(n * width, width)]
        else:
            c, p = (i - up_items) // n_pair, (i - up_items) % n_pair
            src = down_hbm.at[pl.ds(first + 2 * p, 2), :, pl.ds(c * width, width)]
        return pltpu.make_async_copy(src, ring.at[i % RING], ring_sem.at[i % RING])

    def buf(kind, r):
        return (idx_all, gate_all)[kind].at[r] if kind < 2 else xall.at[kind - 2, r]

    loads = [pltpu.make_async_copy(src, buf(k, 0), load_sem.at[k])
             for k, src in enumerate((idx_hbm, gate_hbm, x_hbm.at[:, :half], x_hbm.at[:, half:]))]
    for cp in loads:
        cp.start()
    for i in range(min(RING, items)):
        weight(i).start(priority=1)

    barrier = pltpu.get_barrier_semaphore()
    for dev in [partner] + [chip_dev(k) for k in range(1, chips)]:
        pl.semaphore_signal(barrier, inc=1, device_id=dev, device_id_type=MESH)
    pl.semaphore_wait(barrier, chips)

    started = []

    def remote(kind, src, dst, dev):
        return pltpu.make_async_remote_copy(
            src_ref=buf(kind, src), dst_ref=buf(kind, dst),
            send_sem=msend.at[kind, dst - 1], recv_sem=mrecv.at[kind, dst],
            device_id=dev, device_id_type=MESH)

    def send(kind, src, dst, dev):
        cp = remote(kind, src, dst, dev)
        cp.start()
        started.append(cp)

    def arrived(kind, r):
        remote(kind, r, r, partner).wait_recv()

    def relay(kind, k):
        arrived(kind, 2 * k)
        send(kind, 2 * k, 2 * k + 1, partner)

    far_first = list(range(chips - 1, 0, -1))
    for kind in range(4):
        loads[kind].wait()
        for k in far_first:
            send(kind, 0, 2 * k, chip_dev(k))
        send(kind, 0, 1, partner)
    for kind in range(2):
        for k in range(1, chips):
            relay(kind, k)
    for kind in range(2):
        for k in range(chips):
            arrived(kind, 2 * k + 1)

    row = lax.broadcasted_iota(jnp.int32, (slots, tok), 0)
    eid = row // cap + (expert * n_loc + first)
    pos = (row % cap).astype(jnp.float32)
    before = (lax.broadcasted_iota(jnp.int32, (tok, tok), 0)
              < lax.broadcasted_iota(jnp.int32, (tok, tok), 1)).astype(jnp.bfloat16)
    for r in range(ranks):
        chose = jnp.zeros((slots, tok), jnp.float32)
        gate = jnp.zeros((slots, tok), jnp.float32)
        for j in range(top_k):
            hit = idx_all[r, j:j + 1, :] == eid
            chose = jnp.where(hit, 1.0, chose)
            gate = jnp.where(hit, gate_all[r, j:j + 1, :], gate)
        seen = jnp.dot(chose.astype(jnp.bfloat16), before, preferred_element_type=jnp.float32)
        one = jnp.logical_and(chose > 0.0, seen == pos)
        pmat[r] = jnp.where(one, 1.0, 0.0).astype(jnp.bfloat16)
        comb = jnp.where(one, gate, 0.0).T
        hi = comb.astype(jnp.bfloat16)
        rest = comb - hi.astype(jnp.float32)
        mid = rest.astype(jnp.bfloat16)
        low = (rest - mid.astype(jnp.float32)).astype(jnp.bfloat16)
        cmat[r, 0:tok] = hi
        cmat[r, tok:2 * tok] = mid
        cmat[r, 2 * tok:] = low

    def gather(k, r):
        for s in range(half // SUB):
            cols = slice(s * SUB, (s + 1) * SUB)
            rows = jnp.dot(pmat[r], xall[k, r, :, cols], preferred_element_type=jnp.float32)
            xg[k, :, r * cap:(r + 1) * cap, cols] = rows.astype(jnp.bfloat16).reshape(n_exp, cap, SUB)

    def up_dot(k, p, b, n, cols):
        slot = k * half_items + p * n_up + n
        return jnp.dot(xg[k, 2 * p + b], ring[slot, b, :, cols], preferred_element_type=jnp.float32)

    def up_first(p, carry):
        for b in range(2):
            for n in range(n_up):
                for s in range(width // SUB):
                    cols = slice(s * SUB, (s + 1) * SUB)
                    part[2 * p + b, n, :, cols] = up_dot(0, p, b, n, cols)
        return carry

    def up_second(p, carry):
        for b in range(2):
            for n in range(n_up):
                for s in range(width // SUB):
                    cols = slice(s * SUB, (s + 1) * SUB)
                    acc = part[2 * p + b, n, :, cols] + up_dot(1, p, b, n, cols)
                    hbuf[2 * p + b, n, :, cols] = gelu(acc).astype(jnp.bfloat16)
        return carry

    gather(0, 0)
    arrived(2, 1)
    gather(0, 1)
    gather(1, 0)
    arrived(3, 1)
    gather(1, 1)
    for k in range(1, chips):
        relay(2, k)
        gather(0, 2 * k)
    for k in range(1, chips):
        arrived(2, 2 * k + 1)
        gather(0, 2 * k + 1)
    for i in range(half_items):
        weight(i).wait()
    lax.fori_loop(0, n_pair // 2, up_first, 0, unroll=True)
    for k in range(1, chips):
        relay(3, k)
    lax.fori_loop(n_pair // 2, n_pair, up_first, 0, unroll=True)
    for i in range(RING, min(RING + half_items, items)):
        weight(i).start(priority=1)
    for k in range(1, chips):
        gather(1, 2 * k)
    for k in range(1, chips):
        arrived(3, 2 * k + 1)
        gather(1, 2 * k + 1)
    for i in range(half_items, up_items):
        weight(i).wait()
    lax.fori_loop(0, n_pair, up_second, 0, unroll=True)
    for i in range(RING + half_items, min(RING + up_items, items)):
        weight(i).start(priority=1)

    def d2d(c):
        return pltpu.make_async_remote_copy(
            src_ref=pacc.at[c, 1], dst_ref=d2d_in.at[c],
            send_sem=d2d_send.at[c], recv_sem=d2d_recv.at[c], device_id=partner, device_id_type=MESH)

    lanes = SUB // 2
    order = ((1, 2), (2, 1))

    def ici(c, h, j, src, dst, k):
        return pltpu.make_async_remote_copy(
            src_ref=ssum.at[c, h, src], dst_ref=ici_in.at[c, h, dst],
            send_sem=ici_send.at[c, h, j], recv_sem=ici_recv.at[c, h, j],
            device_id=chip_dev(k), device_id_type=MESH)

    def hop(c, h, j):
        a, b = order[h]
        if c < STAGED:
            return ici(c, h, 0, pl.ds(2, 2), pl.ds(0, 2), a) if j == 0 else ici(c, h, 1, 1, 2, b)
        return ici(c, h, j, j + 1, j, (b, a, 3)[j])

    def n_hops(c):
        return 2 if c < STAGED else 3

    def forward(c):
        d2d(c).wait_recv()
        for h, (a, b) in enumerate(order):
            for slot, k in enumerate((0, b, a, 3)):
                cols = slice(h * lanes, (h + 1) * lanes)
                ssum[c, h, slot] = pacc[c, 0, k, :, cols] + d2d_in[c, k, :, cols]
        if c < STAGED:
            for h in range(2):
                hop(c, h, 0).start()
        else:
            for j in range(2, -1, -1):
                for h in range(2):
                    hop(c, h, j).start()

    def second_hop(c):
        for h in range(2):
            hop(c, h, 0).wait_recv()
            ssum[c, h, 1] = ssum[c, h, 1] + ici_in[c, h, 1]
            hop(c, h, 1).start()

    for c in range(n_chunk):
        wide, s = c * SUB // width, c * SUB % width
        cols = slice(s, s + SUB)
        base = up_items + wide * n_pair
        if s == 0:
            for p in range(n_pair):
                weight(base + p).wait()
        for e in range(n_exp):
            slot = (base + e // 2) % RING
            o = jnp.dot(hbuf[e, 0], ring[slot, e % 2, :width, cols], preferred_element_type=jnp.float32)
            for n in range(1, n_up):
                o += jnp.dot(hbuf[e, n], ring[slot, e % 2, n * width:(n + 1) * width, cols],
                             preferred_element_type=jnp.float32)
            obuf[e] = o.astype(jnp.bfloat16)
        for r in range(ranks):
            o = obuf[:, r * cap:(r + 1) * cap, :].reshape(slots, SUB)
            t = jnp.dot(cmat[r], o, preferred_element_type=jnp.float32)
            pacc[c, r % 2, r // 2] = t[:tok] + t[tok:2 * tok] + t[2 * tok:]
        d2d(c).start()
        if c > 0:
            forward(c - 1)
        if 0 <= c - LAG < STAGED:
            second_hop(c - LAG)
    forward(n_chunk - 1)
    for c in range(n_chunk - LAG, STAGED):
        second_hop(c)

    outs = []
    for c in range(n_chunk):
        for h in range(2):
            if c < STAGED:
                hop(c, h, 1).wait_recv()
                total = ssum[c, h, 0] + ici_in[c, h, 0] + ici_in[c, h, 2]
            else:
                for j in range(3):
                    hop(c, h, j).wait_recv()
                total = ssum[c, h, 0] + ici_in[c, h, 0] + ici_in[c, h, 1] + ici_in[c, h, 2]
            out_v[c, :, h * lanes:(h + 1) * lanes] = total.astype(jnp.bfloat16)
        cp = pltpu.make_async_copy(out_v.at[c], out_hbm.at[:, pl.ds(c * SUB, SUB)], out_sem.at[c])
        cp.start()
        outs.append(cp)
    for cp in started:
        cp.wait_send()
    for c in range(n_chunk):
        d2d(c).wait_send()
        for h in range(2):
            for j in range(n_hops(c)):
                hop(c, h, j).wait_send()
        outs[c].wait()


def solution(mesh):
    pool = POOL

    def local_moe(x_loc, idx_loc, gate_loc, up_loc, down_loc):
        tok, d_model = x_loc.shape
        top_k = idx_loc.shape[1]
        n_loc, _, d_ff = up_loc.shape
        n_all = n_loc * mesh.shape['expert']
        cap = min(4, n_all // top_k) * tok * top_k // n_all
        chips, ranks = 2 * pool, 4 * pool
        n_exp = n_loc // pool
        slots = n_exp * cap
        width = d_ff // 2
        n_chunk = d_model // SUB
        n_up = d_ff // width
        up4 = up_loc.reshape(n_loc, 2, d_model // 2, d_ff)
        dma, f32, bf16 = pltpu.SemaphoreType.DMA, jnp.float32, jnp.bfloat16
        hbm = pl.BlockSpec(memory_space=pltpu.HBM)
        return pl.pallas_call(
            functools.partial(kernel, pool, cap),
            out_shape=jax.ShapeDtypeStruct((tok, d_model), bf16),
            in_specs=[hbm] * 5,
            out_specs=hbm,
            scratch_shapes=[
                pltpu.VMEM((RING, 2, d_ff, width), bf16),
                pltpu.VMEM((2, ranks, tok, d_model // 2), bf16),
                pltpu.VMEM((ranks, top_k, tok), jnp.int32),
                pltpu.VMEM((ranks, top_k, tok), f32),
                pltpu.VMEM((ranks, slots, tok), bf16),
                pltpu.VMEM((ranks, 3 * tok, slots), bf16),
                pltpu.VMEM((2, n_exp, ranks * cap, d_model // 2), bf16),
                pltpu.VMEM((n_exp, n_up, ranks * cap, width), f32),
                pltpu.VMEM((n_exp, n_up, ranks * cap, width), bf16),
                pltpu.VMEM((n_exp, ranks * cap, SUB), bf16),
                pltpu.VMEM((n_chunk, 2, chips, tok, SUB), f32),
                pltpu.VMEM((n_chunk, chips, tok, SUB), f32),
                pltpu.VMEM((n_chunk, 2, chips, tok, SUB // 2), f32),
                pltpu.VMEM((n_chunk, 2, chips - 1, tok, SUB // 2), f32),
                pltpu.VMEM((n_chunk, tok, SUB), bf16),
                dma((RING,)), dma((4,)),
                dma((4, ranks - 1)), dma((4, ranks)),
                dma((n_chunk,)), dma((n_chunk,)),
                dma((n_chunk, 2, chips - 1)), dma((n_chunk, 2, chips - 1)),
                dma((n_chunk,)),
            ],
            compiler_params=pltpu.CompilerParams(
                collective_id=0, has_side_effects=True, vmem_limit_bytes=67043328),
            name="moe",
        )(x_loc, idx_loc.T, gate_loc.T, up4, down_loc)

    tok_spec = P(('data', 'expert'), None)
    w_spec = P('expert', None, None)
    return jax.shard_map(local_moe, mesh=mesh, in_specs=(tok_spec, tok_spec, tok_spec, w_spec, w_spec), out_specs=tok_spec, check_vma=False)
```

```python
import functools

import jax
import jax.numpy as jnp
from jax import lax
from jax.experimental import pallas as pl
from jax.experimental.pallas import tpu as pltpu
from jax.sharding import PartitionSpec as P

MESH = pl.DeviceIdType.MESH
POOL = 2
RING = 20
SUB = 256
STAGED = 7
LAG = 4
GELU_C = 0.7978845608028654


def gelu(v):
    return v * (0.5 + 0.5 * jnp.tanh(v * (GELU_C + (GELU_C * 0.044715) * (v * v))))


def kernel(pool, cap, x_hbm, idx_hbm, gate_hbm, up_hbm, down_hbm, out_hbm,
           ring, xall, idx_all, gate_all, pmat, cmat, xg, part, hbuf, obuf, pacc, d2d_in, ssum, ici_in, out_v,
           ring_sem, load_sem, msend, mrecv, d2d_send, d2d_recv, ici_send, ici_recv, out_sem):
    data, expert = lax.axis_index("data"), lax.axis_index("expert")
    core = expert % 2
    y = data % pool
    chips = 2 * pool
    ranks = 2 * chips
    tok = x_hbm.shape[0]
    top_k = idx_hbm.shape[0]
    n_loc = up_hbm.shape[0]
    n_exp = n_loc // pool
    half, width = ring.shape[2:]
    n_up = up_hbm.shape[3] // width
    n_wide = down_hbm.shape[2] // width
    n_chunk = down_hbm.shape[2] // SUB
    n_pair = n_exp // 2
    half_items = n_pair * n_up
    up_items = 2 * half_items
    items = up_items + n_wide * n_pair
    first = y * n_exp
    slots = n_exp * cap

    partner = (data, expert + 1 - 2 * core)

    def chip_dev(k):
        ex = partner[1] if k % 2 == 0 else lax.rem(partner[1] + 2, 4)
        da = data if k < 2 else data + 1 - 2 * y
        return (da, ex)

    def weight(i):
        if i < up_items:
            k, p, n = i // half_items, i % half_items // n_up, i % n_up
            src = up_hbm.at[pl.ds(first + 2 * p, 2), k, :, pl.ds(n * width, width)]
        else:
            c, p = (i - up_items) // n_pair, (i - up_items) % n_pair
            src = down_hbm.at[pl.ds(first + 2 * p, 2), :, pl.ds(c * width, width)]
        return pltpu.make_async_copy(src, ring.at[i % RING], ring_sem.at[i % RING])

    def buf(kind, r):
        return (idx_all, gate_all)[kind].at[r] if kind < 2 else xall.at[kind - 2, r]

    loads = [pltpu.make_async_copy(src, buf(k, 0), load_sem.at[k])
             for k, src in enumerate((idx_hbm, gate_hbm, x_hbm.at[:, :half], x_hbm.at[:, half:]))]
    for cp in loads:
        cp.start()
    for i in range(min(RING, items)):
        weight(i).start(priority=1)

    barrier = pltpu.get_barrier_semaphore()
    for dev in [partner] + [chip_dev(k) for k in range(1, chips)]:
        pl.semaphore_signal(barrier, inc=1, device_id=dev, device_id_type=MESH)
    pl.semaphore_wait(barrier, chips)

    started = []

    def remote(kind, src, dst, dev):
        return pltpu.make_async_remote_copy(
            src_ref=buf(kind, src), dst_ref=buf(kind, dst),
            send_sem=msend.at[kind, dst - 1], recv_sem=mrecv.at[kind, dst],
            device_id=dev, device_id_type=MESH)

    def send(kind, src, dst, dev):
        cp = remote(kind, src, dst, dev)
        cp.start()
        started.append(cp)

    def arrived(kind, r):
        remote(kind, r, r, partner).wait_recv()

    def relay(kind, k):
        arrived(kind, 2 * k + 1)
        send(kind, 2 * k + 1, 2 * k, partner)

    far_first = list(range(chips - 1, 0, -1))
    for kind in range(4):
        loads[kind].wait()
        for k in far_first:
            send(kind, 0, 2 * k + 1, chip_dev(k))
        send(kind, 0, 1, partner)
    for kind in range(2):
        for k in range(1, chips):
            relay(kind, k)
    for kind in range(2):
        arrived(kind, 1)
        for k in range(1, chips):
            arrived(kind, 2 * k)

    eid = lax.broadcasted_iota(jnp.int32, (n_exp, tok), 0) + (expert * n_loc + first)
    pos = (lax.broadcasted_iota(jnp.int32, (slots, tok), 0) % cap).astype(jnp.float32)
    before = (lax.broadcasted_iota(jnp.int32, (tok, tok), 0)
              < lax.broadcasted_iota(jnp.int32, (tok, tok), 1)).astype(jnp.bfloat16)
    gates = []
    for r in range(ranks):
        gate = jnp.full((n_exp, tok), -1.0)
        for j in range(top_k):
            gate = jnp.where(idx_all[r, j:j + 1, :] == eid, gate_all[r, j:j + 1, :], gate)
        gates.append(gate)
    gates = jnp.concatenate(gates, axis=0)
    chose = jnp.where(gates >= 0.0, 1.0, 0.0)
    seen = jnp.dot(chose.astype(jnp.bfloat16), before, preferred_element_type=jnp.float32)
    place = jnp.where(gates >= 0.0, seen, -1.0)

    def spread(a, r):
        a = a[r * n_exp:(r + 1) * n_exp]
        return jnp.broadcast_to(a[:, None, :], (n_exp, cap, tok)).reshape(slots, tok)

    for r in range(ranks):
        one = spread(place, r) == pos
        pmat[r] = jnp.where(one, 1.0, 0.0).astype(jnp.bfloat16)
        comb = jnp.where(one, spread(gates, r), 0.0).T
        hi = comb.astype(jnp.bfloat16)
        rest = comb - hi.astype(jnp.float32)
        mid = rest.astype(jnp.bfloat16)
        low = (rest - mid.astype(jnp.float32)).astype(jnp.bfloat16)
        cmat[r, 0:tok] = hi
        cmat[r, tok:2 * tok] = mid
        cmat[r, 2 * tok:] = low

    def gather(k, r):
        for s in range(half // SUB):
            cols = slice(s * SUB, (s + 1) * SUB)
            rows = jnp.dot(pmat[r], xall[k, r, :, cols], preferred_element_type=jnp.float32)
            xg[k, :, r * cap:(r + 1) * cap, cols] = rows.astype(jnp.bfloat16).reshape(n_exp, cap, SUB)

    def up_dot(k, p, b, n, cols):
        slot = k * half_items + p * n_up + n
        return jnp.dot(xg[k, 2 * p + b], ring[slot, b, :, cols], preferred_element_type=jnp.float32)

    def up_first(p, carry):
        for b in range(2):
            for n in range(n_up):
                for s in range(width // SUB):
                    cols = slice(s * SUB, (s + 1) * SUB)
                    part[2 * p + b, n, :, cols] = up_dot(0, p, b, n, cols)
        return carry

    def up_second(p, carry):
        for b in range(2):
            for n in range(n_up):
                for s in range(width // SUB):
                    cols = slice(s * SUB, (s + 1) * SUB)
                    acc = part[2 * p + b, n, :, cols] + up_dot(1, p, b, n, cols)
                    hbuf[2 * p + b, n, :, cols] = gelu(acc).astype(jnp.bfloat16)
        return carry

    gather(0, 0)
    arrived(2, 1)
    gather(0, 1)
    gather(1, 0)
    for k in range(1, chips):
        relay(2, k)
    for k in range(1, chips):
        gather(0, 2 * k + 1)
    arrived(3, 1)
    gather(1, 1)
    for k in range(1, chips):
        arrived(2, 2 * k)
    for k in range(1, chips):
        gather(0, 2 * k)
    for i in range(half_items):
        weight(i).wait()
    lax.fori_loop(0, n_pair - 1, up_first, 0, unroll=True)
    for k in range(1, chips):
        relay(3, k)
    lax.fori_loop(n_pair - 1, n_pair, up_first, 0, unroll=True)
    for i in range(RING, min(RING + half_items, items)):
        weight(i).start(priority=1)
    for k in range(1, chips):
        arrived(3, 2 * k)
    for k in range(1, chips):
        gather(1, 2 * k + 1)
        gather(1, 2 * k)
    for i in range(half_items, up_items):
        weight(i).wait()
    lax.fori_loop(0, n_pair, up_second, 0, unroll=True)
    for i in range(RING + half_items, min(RING + up_items, items)):
        weight(i).start(priority=1)

    def d2d(c):
        return pltpu.make_async_remote_copy(
            src_ref=pacc.at[c, 1], dst_ref=d2d_in.at[c],
            send_sem=d2d_send.at[c], recv_sem=d2d_recv.at[c], device_id=partner, device_id_type=MESH)

    lanes = SUB // 2
    order = ((1, 2), (2, 1))

    def ici(c, h, j, src, dst, k):
        return pltpu.make_async_remote_copy(
            src_ref=ssum.at[c, h, src], dst_ref=ici_in.at[c, h, dst],
            send_sem=ici_send.at[c, h, j], recv_sem=ici_recv.at[c, h, j],
            device_id=chip_dev(k), device_id_type=MESH)

    def hop(c, h, j):
        a, b = order[h]
        if c < STAGED:
            return ici(c, h, 0, pl.ds(2, 2), pl.ds(0, 2), a) if j == 0 else ici(c, h, 1, 1, 2, b)
        return ici(c, h, j, j + 1, j, (b, a, 3)[j])

    def n_hops(c):
        return 2 if c < STAGED else 3

    def forward(c):
        d2d(c).wait_recv()
        for h, (a, b) in enumerate(order):
            for slot, k in enumerate((0, b, a, 3)):
                cols = slice(h * lanes, (h + 1) * lanes)
                ssum[c, h, slot] = pacc[c, 0, k, :, cols] + d2d_in[c, k, :, cols]
        if c < STAGED:
            for h in range(2):
                hop(c, h, 0).start()
        else:
            for j in range(2, -1, -1):
                for h in range(2):
                    hop(c, h, j).start()

    def second_hop(c):
        for h in range(2):
            hop(c, h, 0).wait_recv()
            ssum[c, h, 1] = ssum[c, h, 1] + ici_in[c, h, 1]
            hop(c, h, 1).start()

    def side(c, r):
        crossings = (0, 1, 1, 2 if c < STAGED else 1)[r // 2]
        return (r + crossings) % 2

    for c in range(n_chunk):
        wide, s = c * SUB // width, c * SUB % width
        cols = slice(s, s + SUB)
        base = up_items + wide * n_pair
        if s == 0:
            for p in range(n_pair):
                weight(base + p).wait()
        for e in range(n_exp):
            slot = (base + e // 2) % RING
            o = jnp.dot(hbuf[e, 0], ring[slot, e % 2, :width, cols], preferred_element_type=jnp.float32)
            for n in range(1, n_up):
                o += jnp.dot(hbuf[e, n], ring[slot, e % 2, n * width:(n + 1) * width, cols],
                             preferred_element_type=jnp.float32)
            obuf[e] = o.astype(jnp.bfloat16)
        for r in range(ranks):
            o = obuf[:, r * cap:(r + 1) * cap, :].reshape(slots, SUB)
            t = jnp.dot(cmat[r], o, preferred_element_type=jnp.float32)
            pacc[c, side(c, r), r // 2] = t[:tok] + t[tok:2 * tok] + t[2 * tok:]
        d2d(c).start()
        if c > 0:
            forward(c - 1)
        if 0 <= c - LAG < STAGED:
            second_hop(c - LAG)
    forward(n_chunk - 1)
    for c in range(n_chunk - LAG, STAGED):
        second_hop(c)

    outs = []
    for c in range(n_chunk):
        for h in range(2):
            if c < STAGED:
                hop(c, h, 1).wait_recv()
                total = ssum[c, h, 0] + ici_in[c, h, 0] + ici_in[c, h, 2]
            else:
                for j in range(3):
                    hop(c, h, j).wait_recv()
                total = ssum[c, h, 0] + ici_in[c, h, 0] + ici_in[c, h, 1] + ici_in[c, h, 2]
            out_v[c, :, h * lanes:(h + 1) * lanes] = total.astype(jnp.bfloat16)
        cp = pltpu.make_async_copy(out_v.at[c], out_hbm.at[:, pl.ds(c * SUB, SUB)], out_sem.at[c])
        cp.start()
        outs.append(cp)
    for cp in started:
        cp.wait_send()
    for c in range(n_chunk):
        d2d(c).wait_send()
        for h in range(2):
            for j in range(n_hops(c)):
                hop(c, h, j).wait_send()
        outs[c].wait()


def solution(mesh):
    pool = POOL

    def local_moe(x_loc, idx_loc, gate_loc, up_loc, down_loc):
        tok, d_model = x_loc.shape
        top_k = idx_loc.shape[1]
        n_loc, _, d_ff = up_loc.shape
        n_all = n_loc * mesh.shape['expert']
        cap = min(4, n_all // top_k) * tok * top_k // n_all
        chips, ranks = 2 * pool, 4 * pool
        n_exp = n_loc // pool
        slots = n_exp * cap
        width = d_ff // 2
        n_chunk = d_model // SUB
        n_up = d_ff // width
        up4 = up_loc.reshape(n_loc, 2, d_model // 2, d_ff)
        dma, f32, bf16 = pltpu.SemaphoreType.DMA, jnp.float32, jnp.bfloat16
        hbm = pl.BlockSpec(memory_space=pltpu.HBM)
        return pl.pallas_call(
            functools.partial(kernel, pool, cap),
            out_shape=jax.ShapeDtypeStruct((tok, d_model), bf16),
            in_specs=[hbm] * 5,
            out_specs=hbm,
            scratch_shapes=[
                pltpu.VMEM((RING, 2, d_ff, width), bf16),
                pltpu.VMEM((2, ranks, tok, d_model // 2), bf16),
                pltpu.VMEM((ranks, top_k, tok), jnp.int32),
                pltpu.VMEM((ranks, top_k, tok), f32),
                pltpu.VMEM((ranks, slots, tok), bf16),
                pltpu.VMEM((ranks, 3 * tok, slots), bf16),
                pltpu.VMEM((2, n_exp, ranks * cap, d_model // 2), bf16),
                pltpu.VMEM((n_exp, n_up, ranks * cap, width), f32),
                pltpu.VMEM((n_exp, n_up, ranks * cap, width), bf16),
                pltpu.VMEM((n_exp, ranks * cap, SUB), bf16),
                pltpu.VMEM((n_chunk, 2, chips, tok, SUB), f32),
                pltpu.VMEM((n_chunk, chips, tok, SUB), f32),
                pltpu.VMEM((n_chunk, 2, chips, tok, SUB // 2), f32),
                pltpu.VMEM((n_chunk, 2, chips - 1, tok, SUB // 2), f32),
                pltpu.VMEM((n_chunk, tok, SUB), bf16),
                dma((RING,)), dma((4,)),
                dma((4, ranks - 1)), dma((4, ranks)),
                dma((n_chunk,)), dma((n_chunk,)),
                dma((n_chunk, 2, chips - 1)), dma((n_chunk, 2, chips - 1)),
                dma((n_chunk,)),
            ],
            compiler_params=pltpu.CompilerParams(
                collective_id=0, has_side_effects=True, vmem_limit_bytes=67043328),
            name="moe",
        )(x_loc, idx_loc.T, gate_loc.T, up4, down_loc)

    tok_spec = P(('data', 'expert'), None)
    w_spec = P('expert', None, None)
    return jax.shard_map(local_moe, mesh=mesh, in_specs=(tok_spec, tok_spec, tok_spec, w_spec, w_spec), out_specs=tok_spec, check_vma=False)
```

```python
import functools

import jax
import jax.numpy as jnp
from jax import lax
from jax.experimental import pallas as pl
from jax.experimental.pallas import tpu as pltpu
from jax.sharding import PartitionSpec as P

MESH = pl.DeviceIdType.MESH
POOL = 2
RING = 20
SUB = 256
STAGED = 7
LAG = 4
GELU_C = 0.7978845608028654


def gelu(v):
    return v * (0.5 + 0.5 * jnp.tanh(v * (GELU_C + (GELU_C * 0.044715) * (v * v))))


def kernel(pool, cap, x_hbm, idx_hbm, gate_hbm, up_hbm, down_hbm, out_hbm,
           ring, xall, idx_all, gate_all, pmat, cmat, xg, part, hbuf, obuf, pacc, d2d_in, ssum, ici_in, out_v,
           ring_sem, load_sem, msend, mrecv, d2d_send, d2d_recv, ici_send, ici_recv, out_sem):
    data, expert = lax.axis_index("data"), lax.axis_index("expert")
    core = expert % 2
    y = data % pool
    chips = 2 * pool
    ranks = 2 * chips
    tok = x_hbm.shape[0]
    top_k = idx_hbm.shape[0]
    n_loc = up_hbm.shape[0]
    n_exp = n_loc // pool
    half, width = ring.shape[2:]
    n_up = up_hbm.shape[3] // width
    n_wide = down_hbm.shape[2] // width
    n_chunk = down_hbm.shape[2] // SUB
    n_pair = n_exp // 2
    half_items = n_pair * n_up
    up_items = 2 * half_items
    items = up_items + n_wide * n_pair
    first = y * n_exp
    slots = n_exp * cap

    partner = (data, expert + 1 - 2 * core)

    def chip_dev(k):
        ex = partner[1] if k % 2 == 0 else lax.rem(partner[1] + 2, 4)
        da = data if k < 2 else data + 1 - 2 * y
        return (da, ex)

    def weight(i):
        if i < up_items:
            k, p, n = i // half_items, i % half_items // n_up, i % n_up
            src = up_hbm.at[pl.ds(first + 2 * p, 2), k, :, pl.ds(n * width, width)]
        else:
            c, p = (i - up_items) // n_pair, (i - up_items) % n_pair
            src = down_hbm.at[pl.ds(first + 2 * p, 2), :, pl.ds(c * width, width)]
        return pltpu.make_async_copy(src, ring.at[i % RING], ring_sem.at[i % RING])

    def buf(kind, r):
        return (idx_all, gate_all)[kind].at[r] if kind < 2 else xall.at[kind - 2, r]

    loads = [pltpu.make_async_copy(src, buf(k, 0), load_sem.at[k])
             for k, src in enumerate((idx_hbm, gate_hbm, x_hbm.at[:, :half], x_hbm.at[:, half:]))]
    for cp in loads:
        cp.start()
    for i in range(min(RING, items)):
        weight(i).start(priority=1)

    barrier = pltpu.get_barrier_semaphore()
    for dev in [partner] + [chip_dev(k) for k in range(1, chips)]:
        pl.semaphore_signal(barrier, inc=1, device_id=dev, device_id_type=MESH)
    pl.semaphore_wait(barrier, chips)

    started = []

    def remote(kind, src, dst, dev):
        return pltpu.make_async_remote_copy(
            src_ref=buf(kind, src), dst_ref=buf(kind, dst),
            send_sem=msend.at[kind, dst - 1], recv_sem=mrecv.at[kind, dst],
            device_id=dev, device_id_type=MESH)

    def send(kind, src, dst, dev):
        cp = remote(kind, src, dst, dev)
        cp.start()
        started.append(cp)

    def arrived(kind, r):
        remote(kind, r, r, partner).wait_recv()

    def relay(kind, k):
        arrived(kind, 2 * k + 1)
        send(kind, 2 * k + 1, 2 * k, partner)

    far_first = list(range(chips - 1, 0, -1))
    for kind in range(4):
        loads[kind].wait()
        for k in far_first:
            send(kind, 0, 2 * k + 1, chip_dev(k))
        send(kind, 0, 1, partner)
    for kind in range(2):
        for k in range(1, chips):
            relay(kind, k)
    for kind in range(2):
        arrived(kind, 1)
        for k in range(1, chips):
            arrived(kind, 2 * k)

    eid = lax.broadcasted_iota(jnp.int32, (n_exp, tok), 0) + (expert * n_loc + first)
    pos = (lax.broadcasted_iota(jnp.int32, (slots, tok), 0) % cap).astype(jnp.float32)
    before = (lax.broadcasted_iota(jnp.int32, (tok, tok), 0)
              < lax.broadcasted_iota(jnp.int32, (tok, tok), 1)).astype(jnp.bfloat16)
    gates = []
    for r in range(ranks):
        gate = jnp.full((n_exp, tok), -1.0)
        for j in range(top_k):
            gate = jnp.where(idx_all[r, j:j + 1, :] == eid, gate_all[r, j:j + 1, :], gate)
        gates.append(gate)
    gates = jnp.concatenate(gates, axis=0)
    chose = jnp.where(gates >= 0.0, 1.0, 0.0)
    seen = jnp.dot(chose.astype(jnp.bfloat16), before, preferred_element_type=jnp.float32)
    place = jnp.where(gates >= 0.0, seen, -1.0)

    def spread(a, r):
        a = a[r * n_exp:(r + 1) * n_exp]
        return jnp.broadcast_to(a[:, None, :], (n_exp, cap, tok)).reshape(slots, tok)

    for r in range(ranks):
        one = spread(place, r) == pos
        pmat[r] = jnp.where(one, 1.0, 0.0).astype(jnp.bfloat16)
        comb = jnp.where(one, spread(gates, r), 0.0).T
        hi = comb.astype(jnp.bfloat16)
        rest = comb - hi.astype(jnp.float32)
        mid = rest.astype(jnp.bfloat16)
        low = (rest - mid.astype(jnp.float32)).astype(jnp.bfloat16)
        cmat[r, 0:tok] = hi
        cmat[r, tok:2 * tok] = mid
        cmat[r, 2 * tok:] = low

    def gather(k, r):
        for s in range(half // SUB):
            cols = slice(s * SUB, (s + 1) * SUB)
            rows = jnp.dot(pmat[r], xall[k, r, :, cols], preferred_element_type=jnp.float32)
            xg[k, :, r * cap:(r + 1) * cap, cols] = rows.astype(jnp.bfloat16).reshape(n_exp, cap, SUB)

    def up_dot(k, p, b, n, cols):
        slot = k * half_items + p * n_up + n
        return jnp.dot(xg[k, 2 * p + b], ring[slot, b, :, cols], preferred_element_type=jnp.float32)

    def up_first(p, carry):
        for b in range(2):
            for n in range(n_up):
                for s in range(width // SUB):
                    cols = slice(s * SUB, (s + 1) * SUB)
                    part[2 * p + b, n, :, cols] = up_dot(0, p, b, n, cols)
        return carry

    def up_second(p, carry):
        for b in range(2):
            for n in range(n_up):
                for s in range(width // SUB):
                    cols = slice(s * SUB, (s + 1) * SUB)
                    acc = part[2 * p + b, n, :, cols] + up_dot(1, p, b, n, cols)
                    hbuf[2 * p + b, n, :, cols] = gelu(acc).astype(jnp.bfloat16)
        return carry

    gather(0, 0)
    arrived(2, 1)
    gather(0, 1)
    gather(1, 0)
    for k in range(1, chips):
        relay(2, k)
    for k in range(1, chips):
        gather(0, 2 * k + 1)
    arrived(3, 1)
    gather(1, 1)
    for k in range(1, chips):
        arrived(2, 2 * k)
    for k in range(1, chips):
        gather(0, 2 * k)
    for i in range(half_items):
        weight(i).wait()
    lax.fori_loop(0, n_pair // 2, up_first, 0, unroll=True)
    for k in range(1, chips):
        relay(3, k)
    lax.fori_loop(n_pair // 2, n_pair, up_first, 0, unroll=True)
    for i in range(RING, min(RING + half_items, items)):
        weight(i).start(priority=1)
    for k in range(1, chips):
        arrived(3, 2 * k)
    for k in range(1, chips):
        gather(1, 2 * k + 1)
        gather(1, 2 * k)
    for i in range(half_items, up_items):
        weight(i).wait()
    lax.fori_loop(0, n_pair, up_second, 0, unroll=True)
    for i in range(RING + half_items, min(RING + up_items, items)):
        weight(i).start(priority=1)

    def d2d(c):
        return pltpu.make_async_remote_copy(
            src_ref=pacc.at[c, 1], dst_ref=d2d_in.at[c],
            send_sem=d2d_send.at[c], recv_sem=d2d_recv.at[c], device_id=partner, device_id_type=MESH)

    lanes = SUB // 2
    order = ((1, 2), (2, 1))

    def ici(c, h, j, src, dst, k):
        return pltpu.make_async_remote_copy(
            src_ref=ssum.at[c, h, src], dst_ref=ici_in.at[c, h, dst],
            send_sem=ici_send.at[c, h, j], recv_sem=ici_recv.at[c, h, j],
            device_id=chip_dev(k), device_id_type=MESH)

    def hop(c, h, j):
        a, b = order[h]
        if c < STAGED:
            return ici(c, h, 0, pl.ds(2, 2), pl.ds(0, 2), a) if j == 0 else ici(c, h, 1, 1, 2, b)
        return pltpu.make_async_remote_copy(
            src_ref=ssum.at[c, :, j + 1], dst_ref=ici_in.at[c, :, j],
            send_sem=ici_send.at[c, 0, j], recv_sem=ici_recv.at[c, 0, j],
            device_id=chip_dev((2, 1, 3)[j]), device_id_type=MESH)

    def n_hops(c):
        return 2 if c < STAGED else 3

    def forward(c):
        d2d(c).wait_recv()
        for h in range(2):
            a, b = order[h if c < STAGED else 0]
            for slot, k in enumerate((0, b, a, 3)):
                cols = slice(h * lanes, (h + 1) * lanes)
                ssum[c, h, slot] = pacc[c, 0, k, :, cols] + d2d_in[c, k, :, cols]
        if c < STAGED:
            for h in range(2):
                hop(c, h, 0).start()
        else:
            for j in range(2, -1, -1):
                hop(c, 0, j).start()

    def second_hop(c):
        for h in range(2):
            hop(c, h, 0).wait_recv()
            ssum[c, h, 1] = ssum[c, h, 1] + ici_in[c, h, 1]
            hop(c, h, 1).start()

    def side(c, r):
        crossings = (0, 1, 1, 2 if c < STAGED else 1)[r // 2]
        return (r + crossings) % 2

    for c in range(n_chunk):
        wide, s = c * SUB // width, c * SUB % width
        cols = slice(s, s + SUB)
        base = up_items + wide * n_pair
        if s == 0:
            for p in range(n_pair):
                weight(base + p).wait()
        for e in range(n_exp):
            slot = (base + e // 2) % RING
            o = jnp.dot(hbuf[e, 0], ring[slot, e % 2, :width, cols], preferred_element_type=jnp.float32)
            for n in range(1, n_up):
                o += jnp.dot(hbuf[e, n], ring[slot, e % 2, n * width:(n + 1) * width, cols],
                             preferred_element_type=jnp.float32)
            obuf[e] = o.astype(jnp.bfloat16)
        for r in range(ranks):
            o = obuf[:, r * cap:(r + 1) * cap, :].reshape(slots, SUB)
            t = jnp.dot(cmat[r], o, preferred_element_type=jnp.float32)
            pacc[c, side(c, r), r // 2] = t[:tok] + t[tok:2 * tok] + t[2 * tok:]
        d2d(c).start()
        if c > 0:
            forward(c - 1)
        if 0 <= c - LAG < STAGED:
            second_hop(c - LAG)
    forward(n_chunk - 1)
    for c in range(n_chunk - LAG, STAGED):
        second_hop(c)

    outs = []
    for c in range(n_chunk):
        for h in range(2):
            if c < STAGED:
                hop(c, h, 1).wait_recv()
                total = ssum[c, h, 0] + ici_in[c, h, 0] + ici_in[c, h, 2]
            else:
                if h == 0:
                    for j in range(3):
                        hop(c, 0, j).wait_recv()
                total = ssum[c, h, 0] + ici_in[c, h, 0] + ici_in[c, h, 1] + ici_in[c, h, 2]
            out_v[c, :, h * lanes:(h + 1) * lanes] = total.astype(jnp.bfloat16)
        cp = pltpu.make_async_copy(out_v.at[c], out_hbm.at[:, pl.ds(c * SUB, SUB)], out_sem.at[c])
        cp.start()
        outs.append(cp)
    for cp in started:
        cp.wait_send()
    for c in range(n_chunk):
        d2d(c).wait_send()
        for h in range(2 if c < STAGED else 1):
            for j in range(n_hops(c)):
                hop(c, h, j).wait_send()
        outs[c].wait()


def solution(mesh):
    pool = POOL

    def local_moe(x_loc, idx_loc, gate_loc, up_loc, down_loc):
        tok, d_model = x_loc.shape
        top_k = idx_loc.shape[1]
        n_loc, _, d_ff = up_loc.shape
        n_all = n_loc * mesh.shape['expert']
        cap = min(4, n_all // top_k) * tok * top_k // n_all
        chips, ranks = 2 * pool, 4 * pool
        n_exp = n_loc // pool
        slots = n_exp * cap
        width = d_ff // 2
        n_chunk = d_model // SUB
        n_up = d_ff // width
        up4 = up_loc.reshape(n_loc, 2, d_model // 2, d_ff)
        dma, f32, bf16 = pltpu.SemaphoreType.DMA, jnp.float32, jnp.bfloat16
        hbm = pl.BlockSpec(memory_space=pltpu.HBM)
        return pl.pallas_call(
            functools.partial(kernel, pool, cap),
            out_shape=jax.ShapeDtypeStruct((tok, d_model), bf16),
            in_specs=[hbm] * 5,
            out_specs=hbm,
            scratch_shapes=[
                pltpu.VMEM((RING, 2, d_ff, width), bf16),
                pltpu.VMEM((2, ranks, tok, d_model // 2), bf16),
                pltpu.VMEM((ranks, top_k, tok), jnp.int32),
                pltpu.VMEM((ranks, top_k, tok), f32),
                pltpu.VMEM((ranks, slots, tok), bf16),
                pltpu.VMEM((ranks, 3 * tok, slots), bf16),
                pltpu.VMEM((2, n_exp, ranks * cap, d_model // 2), bf16),
                pltpu.VMEM((n_exp, n_up, ranks * cap, width), f32),
                pltpu.VMEM((n_exp, n_up, ranks * cap, width), bf16),
                pltpu.VMEM((n_exp, ranks * cap, SUB), bf16),
                pltpu.VMEM((n_chunk, 2, chips, tok, SUB), f32),
                pltpu.VMEM((n_chunk, chips, tok, SUB), f32),
                pltpu.VMEM((n_chunk, 2, chips, tok, SUB // 2), f32),
                pltpu.VMEM((n_chunk, 2, chips - 1, tok, SUB // 2), f32),
                pltpu.VMEM((n_chunk, tok, SUB), bf16),
                dma((RING,)), dma((4,)),
                dma((4, ranks - 1)), dma((4, ranks)),
                dma((n_chunk,)), dma((n_chunk,)),
                dma((n_chunk, 2, chips - 1)), dma((n_chunk, 2, chips - 1)),
                dma((n_chunk,)),
            ],
            compiler_params=pltpu.CompilerParams(
                collective_id=0, has_side_effects=True, vmem_limit_bytes=67043328),
            name="moe",
        )(x_loc, idx_loc.T, gate_loc.T, up4, down_loc)

    tok_spec = P(('data', 'expert'), None)
    w_spec = P('expert', None, None)
    return jax.shard_map(local_moe, mesh=mesh, in_specs=(tok_spec, tok_spec, tok_spec, w_spec, w_spec), out_specs=tok_spec, check_vma=False)
```
